768 devices in a mesh: ep: 48 (over y_hi, z), tp: 16 (over x, y_lo, core).
Axes of the slice: x: 4, y: 8 (y_hi: 4, y_lo: 2; y = y_hi * 2 + y_lo), z: 12, core: 2. Of those that a mesh axis runs over, the one named last changes fastest.
Arguments:
- tokens: bfloat16 [1536, 6144], P('ep', 'tp'), may hold values from -6 to 6
- expert_ids: int32 [1536, 8], P('ep'), may hold values from 0 to 47, all different within a row; in each aligned block of 32 rows (0 to 31, 32 to 63, ...) at most 10 rows name the same one
- gate_scores: float32 [1536, 8], P('ep'), may hold values from 0.05 to 0.6
- routed_gate: bfloat16 [48, 6144, 2048], P('ep', None, 'tp'), may hold values from -0.078125 to 0.078125
- routed_up: bfloat16 [48, 6144, 2048], P('ep', None, 'tp'), may hold values from -0.078125 to 0.078125
- routed_down: bfloat16 [48, 2048, 6144], P('ep', 'tp'), may hold values from -0.1875 to 0.1875
- shared_gate: bfloat16 [6144, 2048], P(None, 'tp'), may hold values from -0.078125 to 0.078125
- shared_up: bfloat16 [6144, 2048], P(None, 'tp'), may hold values from -0.078125 to 0.078125
- shared_down: bfloat16 [2048, 6144], P('tp'), may hold values from -0.1875 to 0.1875
Outputs:
- moe_out: bfloat16 [1536, 6144], P('ep', 'tp')
The draws below stay inside these ranges and needn't reach their ends.
Inputs may be any that keep to these rules, and one draw needn't show every extreme that they name: `expert_ids`: each row names 8 different experts. Among the 32 rows of one aligned block no expert is named more than 10 times, and in some block one expert is named exactly 10 times.
All inputs are finite; a program needn't handle non-finite values.
Results may differ from the reference program's by a relative error of at most 0.019.
Values may be sent and summed in bfloat16 or wider, within the bound.
No kernel may reach another device: no remote copies, remote signals or barrier semaphores. Data moves between devices by JAX's collectives and lax.ppermute only.
A program may use at most 128 MiB of HBM per device.

```python
import math
import jax
import jax.numpy as jnp
import numpy as np
from jax import lax

D = 6144
FF = 2048
FF_S = 2048
TOPK = 8
TOK_EP = 32
EXPERTS = 48
C = 10
TOKENS = 1536
N_EP = 48
N_TP = 16


def raised(result, own_key, source, target, shards_of, factor):
    def block_of(axis_at):
        return (jnp.arange(result.shape[axis_at]) // (result.shape[axis_at] // shards_of)).reshape((-1,) + (1,) * (result.ndim - 1 - axis_at))

    one_side = jax.random.permutation(own_key, shards_of)[block_of(target)]
    second = (block_of(target) + shards_of // 2) % shards_of
    return jnp.where((block_of(source) == one_side) | (block_of(source) == second), factor * result, result)


def block_levels(rng, dims, cuts, smallest, high):
    loudness, own = 1.0, jax.random.fold_in(rng, 6)
    for dim, blocks in cuts:
        steps = jnp.exp(jax.random.uniform(jax.random.fold_in(own, dim), (blocks,), jnp.float32, smallest / len(cuts), high / len(cuts)))
        loudness = loudness * jnp.repeat(steps, dims[dim] // blocks).reshape([-1 if axis == dim else 1 for axis in range(len(dims))])
    return loudness


def assign_block(own_key, own, number, rows, count, top, reach, slope):
    sequence = jax.random.permutation(own_key, count)
    crowded, common = portions_of(count, rows * top, reach, slope, True), portions_of(count, rows * top, reach, slope, False)
    places = jnp.arange(count)

    def named(tallies, rotation):
        used = int((tallies > 0).sum())
        fixed = max(1, used // 4)
        moved = fixed + (places - fixed + rotation * (used - fixed)) % max(1, count - fixed)
        return jnp.zeros((count,), jnp.int32).at[sequence[jnp.where(places < fixed, places, moved)]].set(jnp.asarray(tallies, jnp.int32))

    tallies = jnp.where(number % 4 == 0, named(crowded, number // 4), named(common, number - number // 4 - 1))
    mixed = jax.random.permutation(jax.random.fold_in(own, 3), count)
    source_of, receiver = mixed[0:count // 2 * 2:2], mixed[1:count // 2 * 2:2]
    room = jnp.minimum(tallies[source_of] - 1, reach - tallies[receiver]) // 2
    room = jnp.where((source_of == sequence[0]) | (receiver == sequence[0]) | (tallies[receiver] == 0), 0, jnp.maximum(room, 0))
    moved = jax.random.randint(jax.random.fold_in(own, 4), (count // 2,), 0, 1 << 20) % (room + 1)
    tallies = tallies.at[source_of].add(-moved).at[receiver].add(moved)
    items = jnp.searchsorted(jnp.cumsum(tallies), jnp.arange(rows * top), side="right").astype(jnp.int32)
    table = items.reshape(top, rows).T
    table = table[jax.random.permutation(jax.random.fold_in(own, 1), rows)]
    rotation = jax.random.randint(jax.random.fold_in(own, 2), (rows, 1), 0, top)
    return jnp.take_along_axis(table, (jnp.arange(top)[None, :] + rotation) % top, axis=1)


def portions_of(amount, total, bound, slope, full):
    weights = [(1 << 20) // math.isqrt(grade ** slope) + 1 for grade in range(1, amount + 1)]
    largest = bound if full else min(bound, max(-(-total // amount), total * weights[0] // sum(weights)))
    least = 1 if total - largest >= amount - 1 else 0
    holding, surplus = [largest] + [least] * (amount - 1), total - largest - least * (amount - 1)
    while surplus > 0:
        candidates = [i for i in range(1, amount) if holding[i] < largest] or [i for i in range(1, amount) if holding[i] < bound]
        pool, budget = sum([weights[i] for i in candidates]), surplus
        for i in candidates:
            extra = min(bound - holding[i], max(1, budget * weights[i] // pool), surplus)
            holding[i] = holding[i] + extra
            surplus = surplus - extra
    return np.array(holding)


def bell_draw(own_key, dims, deviation, reach, cuts=(), kind=jnp.bfloat16):
    values = jax.random.normal(own_key, dims, jnp.float32) * deviation
    if len(cuts) > 0:
        values = block_levels(own_key, dims, cuts, -0.22, 0.18) * values
    return jnp.clip(values, min=-reach, max=reach).astype(kind)


def noise_with(stream_key, extent, scale, limit, cuts, heavy, held_as=jnp.bfloat16):
    array = scale * jax.random.normal(stream_key, extent, jnp.float32)
    if cuts:
        array = array * block_levels(stream_key, extent, cuts, -0.22, 0.18)
    return jnp.clip(raised(array, jax.random.fold_in(stream_key, 3), *heavy), -limit, limit).astype(held_as)


def setup_inputs(seed: int = 0) -> dict:
    key_list = jax.random.split(jax.random.key(seed), 10)
    tokens = bell_draw(key_list[0], (TOKENS, D), 1.0, 6.0, ((0, 48), (1, 16)))
    expert_ids_keys = jax.random.split(jax.random.fold_in(key_list[1], 1), TOKENS // TOK_EP)
    expert_ids_turns = jax.random.permutation(jax.random.fold_in(key_list[1], 3), TOKENS // TOK_EP)
    expert_ids = jax.vmap(lambda own, number: assign_block(jax.random.fold_in(key_list[1], 2), own, number, TOK_EP, EXPERTS, TOPK, C, 2))(expert_ids_keys, expert_ids_turns).reshape((TOKENS, TOPK))
    gate_scores = jnp.clip(0.05 + 0.55 * jax.random.uniform(key_list[2], (TOKENS, TOPK), jnp.float32) ** block_levels(key_list[2], (TOKENS, TOPK), ((0, 48),), -0.2, 0.2), 0.05, 0.6)
    routed_gate = bell_draw(key_list[3], (EXPERTS, D, FF), D ** -0.5, 0.078125, ((0, 48), (2, 16)))
    routed_up = bell_draw(key_list[4], (EXPERTS, D, FF), D ** -0.5, 0.078125, ((0, 48), (2, 16)))
    routed_down = noise_with(key_list[5], (EXPERTS, FF, D), FF ** -0.5, 0.1875, ((0, 48), (1, 16)), (1, 2, 16, 2.0))
    shared_gate = bell_draw(key_list[6], (D, FF_S), D ** -0.5, 0.078125, ((1, 16),))
    shared_up = bell_draw(key_list[7], (D, FF_S), D ** -0.5, 0.078125, ((1, 16),))
    shared_down = noise_with(key_list[8], (FF_S, D), FF_S ** -0.5, 0.1875, ((0, 16),), (0, 1, 16, 2.0))
    return {"tokens": tokens, "expert_ids": expert_ids, "gate_scores": gate_scores, "routed_gate": routed_gate, "routed_up": routed_up, "routed_down": routed_down, "shared_gate": shared_gate, "shared_up": shared_up, "shared_down": shared_down}


def routing(expert_ids, gate_scores, experts, capacity):
    row_count, top_count = expert_ids.shape
    entries = expert_ids.reshape(-1).astype(jnp.int32)
    onehot = (entries[:, None] == jnp.arange(experts, dtype=jnp.int32)[None, :]).astype(jnp.int32)
    before = jnp.cumsum(onehot, axis=0, dtype=jnp.int32) - onehot
    slot_rank = jnp.sum(before * onehot, axis=1).astype(jnp.int32)
    position = (entries * capacity + slot_rank).astype(jnp.int32)
    places = (jnp.arange(experts * capacity, dtype=jnp.int32)[:, None] == position[None, :])
    places = places.reshape(experts * capacity, row_count, top_count).astype(jnp.float32)
    select = jnp.sum(places, axis=2).astype(jnp.bfloat16)
    combine_weights = jnp.sum(places * gate_scores[None, :, :].astype(jnp.float32), axis=2)
    return select, combine_weights


def expert_pass(bucket_rows, w_gate, w_up, w_down):
    gate_sum = jnp.dot(bucket_rows, w_gate, preferred_element_type=jnp.float32)
    up_sum = jnp.dot(bucket_rows, w_up, preferred_element_type=jnp.float32)
    hidden = (jax.nn.silu(gate_sum) * up_sum).astype(jnp.bfloat16)
    row_count, hidden_width = hidden.shape
    group_width = hidden_width // N_TP
    hidden_groups = hidden.reshape(row_count, N_TP, group_width).transpose(1, 0, 2)
    down_groups = w_down.reshape(N_TP, group_width, w_down.shape[1])

    def add_group(total, pieces):
        partial_value = jnp.dot(pieces[0], pieces[1], preferred_element_type=jnp.float32)
        return total + partial_value.astype(jnp.bfloat16).astype(jnp.float32), None

    start = jnp.zeros((row_count, w_down.shape[1]), jnp.float32)
    total, unused = lax.scan(add_group, start, (hidden_groups, down_groups))
    return total


def reference(tokens, expert_ids, gate_scores, routed_gate, routed_up, routed_down, shared_gate, shared_up, shared_down):
    block_tokens = tokens.reshape(N_EP, TOK_EP, D)
    block_ids = expert_ids.reshape(N_EP, TOK_EP, TOPK)
    block_scores = gate_scores.reshape(N_EP, TOK_EP, TOPK)

    def fill_buckets(inputs):
        select, combine_weights = routing(inputs[1], inputs[2], EXPERTS, C)
        filled = jnp.dot(select, inputs[0], preferred_element_type=jnp.float32).astype(jnp.bfloat16)
        return filled, combine_weights

    buckets, weights = lax.map(fill_buckets, (block_tokens, block_ids, block_scores))
    by_expert = buckets.reshape(N_EP, EXPERTS, C, D).transpose(1, 0, 2, 3).reshape(EXPERTS, N_EP * C, D)

    def run_expert(inputs):
        return expert_pass(inputs[0], inputs[1], inputs[2], inputs[3]).astype(jnp.bfloat16)

    outputs = lax.map(run_expert, (by_expert, routed_gate, routed_up, routed_down))
    returned = outputs.reshape(EXPERTS, N_EP, C, D).transpose(1, 0, 2, 3).reshape(N_EP, EXPERTS * C, D)
    routed = jnp.einsum("spt,spd->std", weights, returned.astype(jnp.float32), precision=lax.Precision.HIGHEST)
    shared = expert_pass(tokens, shared_gate, shared_up, shared_down)
    return (routed.reshape(TOKENS, D) + shared).astype(jnp.bfloat16)
```

```python
import jax
import jax.numpy as jnp
from jax import lax
from jax.experimental import pallas as pl
from jax.experimental.pallas import tpu as pltpu
from jax.sharding import Mesh
from jax.sharding import PartitionSpec as P

LANES = 128


def slot_table(expert_ids, gate_scores, experts, copies):
    rows = expert_ids.shape[0]
    hit = expert_ids.T[None, :, :] == jnp.arange(experts, dtype=jnp.int32)[:, None, None]
    named = jnp.sum(hit.astype(jnp.float32), axis=1)
    score = jnp.sum(jnp.where(hit, gate_scores.T[None, :, :], 0.0), axis=1)
    earlier = jnp.arange(rows)[:, None] < jnp.arange(rows)[None, :]
    same = jnp.arange(rows)[:, None] == jnp.arange(rows)[None, :]
    weight = jnp.tile(earlier.astype(jnp.bfloat16) + 128 * same.astype(jnp.bfloat16), (1, copies))
    slot = jnp.dot(named.astype(jnp.bfloat16), weight, preferred_element_type=jnp.float32) - 128
    return slot.astype(jnp.int32), jnp.tile(score, (1, copies))


def ffn_kernel(steps, routed_rows, x, wg, wgp, wu, wup, sg, su, wd, wdp, sd, out, acc, sacc, hid, shid):
    i = pl.program_id(0)

    def wide(ref):
        parts = [
            jnp.concatenate([ref[p, j] for j in range(ref.shape[1])], axis=1) for p in range(ref.shape[0])
        ]
        return jnp.concatenate(parts, axis=1)

    @pl.when(i == 0)
    def _():
        acc[...] = jnp.zeros_like(acc)
        sacc[...] = jnp.zeros_like(sacc)

    @pl.when(i < steps)
    def _():
        rows = wide(x)
        w = jnp.concatenate([wg[...], wgp[...], wu[...], wup[...]], axis=1)
        acc[...] += jnp.dot(rows[:routed_rows], w, preferred_element_type=jnp.float32)
        ws = jnp.concatenate([sg[...], su[...]], axis=1)
        sacc[...] += jnp.dot(rows[routed_rows:], ws, preferred_element_type=jnp.float32)

    @pl.when(i == steps)
    def _():
        half = acc.shape[1] // 2
        hid[...] = (jax.nn.silu(acc[:, :half]) * acc[:, half:]).astype(jnp.bfloat16)
        shalf = sacc.shape[1] // 2
        shid[...] = (jax.nn.silu(sacc[:, :shalf]) * sacc[:, shalf:]).astype(jnp.bfloat16)

    @pl.when(i >= steps)
    def _():
        w = jnp.concatenate([wd[...], wdp[...]], axis=0)
        y = jnp.dot(hid[...], w, preferred_element_type=jnp.float32).astype(jnp.bfloat16)
        ys = jnp.dot(shid[...], sd[...], preferred_element_type=jnp.float32).astype(jnp.bfloat16)
        chunks = out.shape[1]
        for p in range(out.shape[0]):
            for j in range(chunks):
                at = (p * chunks + j) * LANES
                out[p, j, :routed_rows] = y[:, at : at + LANES]
                out[p, j, routed_rows:] = ys[:, at : at + LANES]


def ffn(x, own, partner, shared, routed_rows):
    chips, chunks, rows, _ = x.shape
    hidden = own[0].shape[1]
    per = 2
    steps = chips // per
    wide = per * chunks * LANES
    first = lambda i: jnp.minimum(i, steps - 1)
    second = lambda i: jnp.maximum(i - steps, 0)
    w_in = pl.BlockSpec((wide, hidden), lambda i: (first(i), 0))
    w_out = pl.BlockSpec((hidden, wide), lambda i: (0, second(i)))
    x_in = pl.BlockSpec((per, chunks, rows, LANES), lambda i: (first(i), 0, 0, 0))
    x_out = pl.BlockSpec((per, chunks, rows, LANES), lambda i: (second(i), 0, 0, 0))
    shared_rows = rows - routed_rows

    def body(*refs):
        ffn_kernel(steps, routed_rows, *refs)

    return pl.pallas_call(
        body,
        grid=(2 * steps,),
        in_specs=[x_in, w_in, w_in, w_in, w_in, w_in, w_in, w_out, w_out, w_out],
        out_specs=x_out,
        out_shape=jax.ShapeDtypeStruct(x.shape, jnp.bfloat16),
        scratch_shapes=[
            pltpu.VMEM((routed_rows, 4 * hidden), jnp.float32),
            pltpu.VMEM((shared_rows, 2 * hidden), jnp.float32),
            pltpu.VMEM((routed_rows, 2 * hidden), jnp.bfloat16),
            pltpu.VMEM((shared_rows, hidden), jnp.bfloat16),
        ],
        compiler_params=pltpu.CompilerParams(
            dimension_semantics=("arbitrary",), vmem_limit_bytes=48 * 1024 * 1024
        ),
        name="ffn",
    )(x, own[0], partner[0], own[1], partner[1], shared[0], shared[1], own[2], partner[2], shared[2])


def local(
    tokens,
    expert_ids,
    gate_scores,
    routed_gate,
    routed_up,
    routed_down,
    shared_gate,
    shared_up,
    shared_down,
):
    experts = routed_gate.shape[0] * lax.axis_size("ep")
    chips = lax.axis_size("t")
    core = lax.axis_index("c")
    row_count, top_count = expert_ids.shape
    capacity = min(row_count, row_count * top_count * 15 // (8 * experts))
    slots = capacity // 2
    swap = [(0, 1), (1, 0)]
    own = (routed_gate[0], routed_up[0], routed_down[0])
    partner = tuple(lax.ppermute(w, "c", swap) for w in own)

    width = 2 * tokens.shape[1]
    chunks = width // LANES
    message = -(-chunks * slots // 8) * 8
    pair = lax.all_gather(tokens, "c", axis=1, tiled=True)
    stacked = jnp.moveaxis(pair.reshape(row_count, chunks, LANES), 1, 0)
    slot, score = slot_table(expert_ids, gate_scores, experts, chunks)
    place = jnp.arange(message, dtype=jnp.int32)[:, None]
    column = jnp.arange(chunks * row_count, dtype=jnp.int32)[None, :]
    fits = (place // slots == column // row_count) & (place < chunks * slots)
    target = jnp.where(fits, place % slots + slots * core, -1024)
    match = slot[:, None, :] == target[None, :, :]
    select = match.astype(jnp.bfloat16).reshape(experts * message, chunks * row_count)
    buckets = jnp.dot(
        select, stacked.reshape(chunks * row_count, LANES), preferred_element_type=jnp.float32
    ).astype(jnp.bfloat16)
    received = lax.all_to_all(
        buckets.reshape(experts, message, LANES), "ep", split_axis=0, concat_axis=0, tiled=True
    )

    routed_rows = slots * experts
    rows = jnp.swapaxes(received, 0, 1)[: chunks * slots].reshape(chunks, routed_rows, LANES)
    block = jnp.concatenate([rows, stacked], axis=1)
    whole = lax.all_to_all(
        jnp.broadcast_to(block[None], (chips,) + block.shape), "t", split_axis=0, concat_axis=0, tiled=True
    )
    partial = ffn(whole, own, partner, (shared_gate, shared_up, shared_down), routed_rows)
    parts = lax.all_to_all(partial, "t", split_axis=0, concat_axis=0, tiled=True)
    total = jnp.sum(parts.astype(jnp.float32), axis=0)

    outcome = total[:, :routed_rows].astype(jnp.bfloat16).reshape(chunks * slots, experts, LANES)
    outcome = jnp.pad(outcome, ((0, message - chunks * slots), (0, 0), (0, 0)))
    returned = lax.all_to_all(
        jnp.swapaxes(outcome, 0, 1), "ep", split_axis=0, concat_axis=0, tiled=True
    ).reshape(experts * message, LANES)
    weights = jnp.where(match, score[:, None, :], 0.0).reshape(experts * message, chunks * row_count)
    routed = lax.dot_general(
        weights,
        returned.astype(jnp.float32),
        (((0,), (0,)), ((), ())),
        precision=lax.Precision.HIGHEST,
        preferred_element_type=jnp.float32,
    ).reshape(chunks, row_count, LANES)
    both = (routed + total[:, routed_rows:]).reshape(2, chunks // 2, row_count, LANES)
    mine = lax.dynamic_index_in_dim(both, core, 0, keepdims=False)
    other = lax.dynamic_index_in_dim(both, 1 - core, 0, keepdims=False)
    result = mine + lax.ppermute(other, "c", swap)
    return jnp.moveaxis(result, 0, 1).reshape(row_count, tokens.shape[1]).astype(jnp.bfloat16)


def solution(mesh):
    ep, tp = mesh.shape["ep"], mesh.shape["tp"]
    fine = Mesh(mesh.devices.reshape(ep, tp // 2, 2), ("ep", "t", "c"))
    tp_axes = ("t", "c")
    placed = (
        P("ep", tp_axes),
        P("ep", None),
        P("ep", None),
        P("ep", None, tp_axes),
        P("ep", None, tp_axes),
        P("ep", tp_axes, None),
        P(None, tp_axes),
        P(None, tp_axes),
        P(tp_axes, None),
    )
    return jax.shard_map(
        local, mesh=fine, in_specs=placed, out_specs=P("ep", tp_axes), check_vma=False
    )
```

```python
import jax
import jax.numpy as jnp
from jax import lax
from jax.experimental import pallas as pl
from jax.experimental.pallas import tpu as pltpu
from jax.sharding import Mesh
from jax.sharding import PartitionSpec as P


LANES = 128
PARAMS = pltpu.CompilerParams(dimension_semantics=("arbitrary",), vmem_limit_bytes=60 * 1024 * 1024)


def slot_table(expert_ids, gate_scores, experts, copies):
    rows = expert_ids.shape[0]
    hit = expert_ids.T[None, :, :] == jnp.arange(experts, dtype=jnp.int32)[:, None, None]
    named = jnp.sum(hit.astype(jnp.float32), axis=1)
    score = jnp.sum(jnp.where(hit, gate_scores.T[None, :, :], 0.0), axis=1)
    earlier = jnp.arange(rows)[:, None] < jnp.arange(rows)[None, :]
    same = jnp.arange(rows)[:, None] == jnp.arange(rows)[None, :]
    weight = jnp.tile(earlier.astype(jnp.bfloat16) + 128 * same.astype(jnp.bfloat16), (1, copies))
    slot = jnp.dot(named.astype(jnp.bfloat16), weight, preferred_element_type=jnp.float32) - 128
    return slot.astype(jnp.int32), jnp.tile(score, (1, copies))


def activate(total):
    half = total.shape[1] // 2
    return (jax.nn.silu(total[:, :half]) * total[:, half:]).astype(jnp.bfloat16)


def estimate(flops):
    return pl.CostEstimate(flops=flops, bytes_accessed=flops // 400, transcendentals=0)


def split_weights(y, w_gate, w_up, w_down, count, width):
    hidden = w_gate.shape[1]

    def body(_, gm, go, um, uo, dm, do, mine, other, mine_down, other_down):
        mine[0] = gm[...]
        mine[1] = um[...]
        other[0] = go[...]
        other[1] = uo[...]
        mine_down[...] = dm[...]
        other_down[...] = do[...]

    near = pl.BlockSpec((width, hidden), lambda i, y: (2 * i + y[0], 0))
    far = pl.BlockSpec((width, hidden), lambda i, y: (2 * i + 1 - y[0], 0))
    near_down = pl.BlockSpec((hidden, width), lambda i, y: (0, 2 * i + y[0]))
    far_down = pl.BlockSpec((hidden, width), lambda i, y: (0, 2 * i + 1 - y[0]))
    pair = pl.BlockSpec((2, width, hidden), lambda i, y: (0, i, 0))
    column = pl.BlockSpec((hidden, width), lambda i, y: (0, i))
    pair_shape = jax.ShapeDtypeStruct((2, count * width, hidden), w_gate.dtype)
    column_shape = jax.ShapeDtypeStruct((hidden, count * width), w_gate.dtype)
    return pl.pallas_call(
        body,
        grid_spec=pltpu.PrefetchScalarGridSpec(
            num_scalar_prefetch=1,
            grid=(count,),
            in_specs=[near, far, near, far, near_down, far_down],
            out_specs=[pair, pair, column, column],
        ),
        out_shape=[pair_shape, pair_shape, column_shape, column_shape],
        cost_estimate=estimate(10**9),
        compiler_params=PARAMS,
        name="split",
    )(y[None], w_gate, w_gate, w_up, w_up, w_down, w_down)


def partial_sums(x, ins):
    chips, chunks, rows, _ = x.shape
    hidden = ins[0].shape[2]
    width = chunks * LANES
    wide = 2 * len(ins) * hidden

    def body(x_ref, *refs):
        w, acc, sent = refs[: len(ins)], refs[-2], refs[-1]
        i = pl.program_id(0)

        @pl.when(i == 0)
        def _():
            acc[...] = jnp.zeros_like(acc)

        lines = jnp.concatenate([x_ref[0, j] for j in range(chunks)], axis=1)
        weights = jnp.concatenate([r[k] for k in range(2) for r in w], axis=1)
        acc[...] += jnp.dot(lines, weights, preferred_element_type=jnp.float32)

        @pl.when(i == chips - 1)
        def _():
            sent[...] = acc[...].astype(sent.dtype)

    whole = pl.BlockSpec((rows, wide), lambda i: (0, 0))
    return pl.pallas_call(
        body,
        grid=(chips,),
        in_specs=[pl.BlockSpec((1, chunks, rows, LANES), lambda i: (i, 0, 0, 0))]
        + [pl.BlockSpec((2, width, hidden), lambda i: (0, i, 0))] * len(ins),
        out_specs=[whole, whole],
        out_shape=[
            jax.ShapeDtypeStruct((rows, wide), jnp.float32),
            jax.ShapeDtypeStruct((rows, wide), jnp.bfloat16),
        ],
        cost_estimate=estimate(2 * rows * chips * width * wide),
        compiler_params=PARAMS,
        name="partial",
    )(x, *ins)


def down(sums, other, outs, count, chunks):
    rows, wide = sums.shape
    part = outs[0].shape[0]
    width = chunks * LANES

    def body(s_ref, o_ref, *refs):
        w, out, h = refs[: len(outs)], refs[-2], refs[-1]

        @pl.when(pl.program_id(0) == 0)
        def _():
            theirs = o_ref[...].astype(jnp.float32)
            quarter = wide // 4
            order = [1, 0, 3, 2]
            theirs = jnp.concatenate([theirs[:, q * quarter : (q + 1) * quarter] for q in order], axis=1)
            h[...] = activate(s_ref[...] + theirs)

        weights = jnp.concatenate([r[...] for r in w], axis=0)
        result = jnp.dot(h[...], weights, preferred_element_type=jnp.float32)
        for j in range(chunks):
            out[0, j] = result[:, j * LANES : (j + 1) * LANES].astype(out.dtype)

    whole = pl.BlockSpec((rows, wide), lambda i: (0, 0))
    return pl.pallas_call(
        body,
        grid=(count,),
        in_specs=[whole, whole] + [pl.BlockSpec((part, width), lambda i: (0, i))] * len(outs),
        out_specs=pl.BlockSpec((1, chunks, rows, LANES), lambda i: (i, 0, 0, 0)),
        out_shape=jax.ShapeDtypeStruct((count, chunks, rows, LANES), jnp.bfloat16),
        scratch_shapes=[pltpu.VMEM((rows, wide // 2), jnp.bfloat16)],
        cost_estimate=estimate(2 * rows * count * width * 4 * part),
        compiler_params=PARAMS,
        name="down",
    )(sums, other, *outs)


def shared_expert(x, at, w_gate, w_up, w_down):
    pairs, ys, chunks, rows, _ = x.shape
    hidden = w_gate.shape[1]
    width = ys * chunks * LANES

    def body(_, x_ref, g_ref, u_ref, d_ref, out, acc, h):
        i = pl.program_id(0)

        @pl.when(i == 0)
        def _():
            acc[...] = jnp.zeros_like(acc)

        @pl.when(i < pairs)
        def _():
            lines = jnp.concatenate([x_ref[0, y, j] for y in range(ys) for j in range(chunks)], axis=1)
            weights = jnp.concatenate([g_ref[...], u_ref[...]], axis=1)
            acc[...] += jnp.dot(lines, weights, preferred_element_type=jnp.float32)

        @pl.when(i == pairs)
        def _():
            h[...] = activate(acc[...])

        @pl.when(i >= pairs)
        def _():
            result = jnp.dot(h[...], d_ref[...], preferred_element_type=jnp.float32)
            for y in range(ys):
                for j in range(chunks):
                    lane = (y * chunks + j) * LANES
                    out[0, y, j] = result[:, lane : lane + LANES].astype(out.dtype)

    first = lambda i: jnp.minimum(i, pairs - 1)
    second = lambda i: jnp.maximum(i - pairs, 0)
    w_in = pl.BlockSpec((width, hidden), lambda i, at: (at[first(i)], 0))
    block = (1, ys, chunks, rows, LANES)
    return pl.pallas_call(
        body,
        grid_spec=pltpu.PrefetchScalarGridSpec(
            num_scalar_prefetch=1,
            grid=(2 * pairs,),
            in_specs=[
                pl.BlockSpec(block, lambda i, at: (first(i), 0, 0, 0, 0)),
                w_in,
                w_in,
                pl.BlockSpec((hidden, width), lambda i, at: (0, at[second(i)])),
            ],
            out_specs=pl.BlockSpec(block, lambda i, at: (second(i), 0, 0, 0, 0)),
            scratch_shapes=[pltpu.VMEM((rows, 2 * hidden), jnp.float32), pltpu.VMEM((rows, hidden), jnp.bfloat16)],
        ),
        out_shape=jax.ShapeDtypeStruct(x.shape, jnp.bfloat16),
        cost_estimate=estimate(6 * rows * pairs * width * hidden),
        compiler_params=PARAMS,
        name="shared",
    )(at, x, w_gate, w_up, w_down)


def local(
    tokens,
    expert_ids,
    gate_scores,
    routed_gate,
    routed_up,
    routed_down,
    shared_gate,
    shared_up,
    shared_down,
):
    experts = routed_gate.shape[0] * lax.axis_size("ep")
    xs = lax.axis_size("x")
    core, xi, yi = lax.axis_index("c"), lax.axis_index("x"), lax.axis_index("y")
    row_count, top_count = expert_ids.shape
    capacity = min(row_count, row_count * top_count * 15 // (8 * experts))
    slots = capacity // 2
    swap = [(0, 1), (1, 0)]

    def to_y(v):
        return lax.ppermute(v, "y", swap)

    def to_x(v, bit):
        return lax.ppermute(v, "x", [(i, i ^ bit) for i in range(xs)])

    def to_c(v):
        return lax.ppermute(v, "c", swap)

    def halve(v, bit):
        half = v.shape[0] // 2
        return (v[:half].astype(jnp.float32) + to_x(v[half:], bit).astype(jnp.float32)).astype(v.dtype)

    def exchange(v, axes):
        return lax.all_to_all(v, axes, split_axis=0, concat_axis=0, tiled=True)

    chunks = 2 * tokens.shape[1] // LANES
    used = chunks * slots
    message = -(-used // 8) * 8
    columns = chunks * row_count
    routed_rows = slots * experts
    width = chunks * LANES

    pair = lax.all_gather(tokens, "c", axis=1, tiled=True)
    stacked = jnp.moveaxis(pair.reshape(row_count, chunks, LANES), 1, 0)
    slot, score = slot_table(expert_ids, gate_scores, experts, chunks)
    place = jnp.arange(message, dtype=jnp.int32)[:, None]
    column = jnp.arange(columns, dtype=jnp.int32)[None, :]
    fits = (place // slots == column // row_count) & (place < used)
    target = jnp.where(fits, place % slots + slots * core, -1024)
    match = slot[:, None, :] == target[None, :, :]
    select = match.astype(jnp.bfloat16).reshape(experts * message, columns)
    buckets = jnp.dot(select, stacked.reshape(columns, LANES), preferred_element_type=jnp.float32)
    buckets = buckets.astype(jnp.bfloat16).reshape(experts, message, LANES)
    received = exchange(buckets, "ep")

    _, w_gate, w_up, w_down, ours = lax.optimization_barrier(
        (buckets, routed_gate[0], routed_up[0], routed_down[0], stacked)
    )
    theirs = to_y(ours)
    mine, other, mine_down, other_down = split_weights(yi, w_gate, w_up, w_down, xs, width)
    got = to_y(other)
    partner = to_c(mine)
    partner_down = to_c(mine_down)
    whole = jnp.where(yi == 0, jnp.stack([ours, theirs]), jnp.stack([theirs, ours]))[None]
    whole = jnp.concatenate([whole, to_x(whole, 2)], axis=0)
    received, partner, partner_down, whole = lax.optimization_barrier(
        (received, partner, partner_down, whole)
    )
    rows = jnp.swapaxes(received, 0, 1)[:used].reshape(chunks, routed_rows, LANES)
    gathered = exchange(jnp.broadcast_to(rows[None], (xs,) + rows.shape), "x")
    got_down = to_y(other_down)
    partner_got = to_c(got)
    gathered, partner_got = lax.optimization_barrier((gathered, partner_got))
    sums, sent = partial_sums(gathered, (mine, partner, got, partner_got))
    other_sums = to_y(sent)
    whole = jnp.concatenate([whole, to_x(whole, 1)], axis=0)
    partner_got_down = to_c(got_down)
    other_sums, partner_got_down, whole = lax.optimization_barrier((other_sums, partner_got_down, whole))
    products = down(sums, other_sums, (mine_down, partner_down, got_down, partner_got_down), xs, chunks)
    reduced = exchange(products, "x")
    at = jnp.bitwise_xor(jnp.array([0, 2, 1, 3], jnp.int32), xi)
    part = shared_expert(whole, at, shared_gate, shared_up, shared_down)
    reduced, part = lax.optimization_barrier((reduced, part))
    total = jnp.sum(reduced.astype(jnp.float32), axis=0).astype(jnp.bfloat16)
    outcome = jnp.pad(total.reshape(used, experts, LANES), ((0, message - used), (0, 0), (0, 0)))
    returned = exchange(jnp.swapaxes(outcome, 0, 1), "ep")
    part = halve(part, 1)
    part = halve(part, 2)[0]
    kept = jnp.where(yi == 0, part[0], part[1])
    lost = jnp.where(yi == 0, part[1], part[0])
    shared = kept.astype(jnp.float32) + to_y(lost).astype(jnp.float32)
    returned, shared = lax.optimization_barrier((returned, shared))

    returned = returned.reshape(experts * message, LANES)
    weights = jnp.where(match, score[:, None, :], 0.0).reshape(experts * message, columns)
    routed = lax.dot_general(
        weights,
        returned.astype(jnp.float32),
        (((0,), (0,)), ((), ())),
        precision=lax.Precision.HIGHEST,
        preferred_element_type=jnp.float32,
    )
    both = (routed.reshape(shared.shape) + shared).reshape(2, chunks // 2, row_count, LANES)
    keep = jnp.where(core == 0, both[0], both[1])
    send = jnp.where(core == 0, both[1], both[0])
    result = keep + lax.ppermute(send, "c", swap)
    return jnp.moveaxis(result, 0, 1).reshape(row_count, tokens.shape[1]).astype(jnp.bfloat16)


def solution(mesh):
    ep, tp = mesh.shape["ep"], mesh.shape["tp"]
    fine = Mesh(mesh.devices.reshape(ep, tp // 4, 2, 2), ("ep", "x", "y", "c"))
    tp_axes = ("x", "y", "c")
    placed = (
        P("ep", tp_axes),
        P("ep", None),
        P("ep", None),
        P("ep", None, tp_axes),
        P("ep", None, tp_axes),
        P("ep", tp_axes, None),
        P(None, tp_axes),
        P(None, tp_axes),
        P(tp_axes, None),
    )
    return jax.shard_map(
        local, mesh=fine, in_specs=placed, out_specs=P("ep", tp_axes), check_vma=False
    )
```

```python
import jax
import jax.numpy as jnp
from jax import lax
from jax.experimental import pallas as pl
from jax.experimental.pallas import tpu as pltpu
from jax.sharding import Mesh
from jax.sharding import PartitionSpec as P


LANES = 128
SMALL = pltpu.CompilerParams(dimension_semantics=("arbitrary",), vmem_limit_bytes=24 * 1024 * 1024)
PARAMS = pltpu.CompilerParams(dimension_semantics=("arbitrary",), vmem_limit_bytes=60 * 1024 * 1024)


def slot_table(expert_ids, gate_scores, experts, copies):
    rows = expert_ids.shape[0]
    hit = expert_ids.T[None, :, :] == jnp.arange(experts, dtype=jnp.int32)[:, None, None]
    named = jnp.sum(hit.astype(jnp.float32), axis=1)
    score = jnp.sum(jnp.where(hit, gate_scores.T[None, :, :], 0.0), axis=1)
    earlier = jnp.arange(rows)[:, None] < jnp.arange(rows)[None, :]
    same = jnp.arange(rows)[:, None] == jnp.arange(rows)[None, :]
    weight = jnp.tile(earlier.astype(jnp.bfloat16) + 128 * same.astype(jnp.bfloat16), (1, copies))
    slot = jnp.dot(named.astype(jnp.bfloat16), weight, preferred_element_type=jnp.float32) - 128
    return slot.astype(jnp.int32), jnp.tile(score, (1, copies))


def activate(total):
    half = total.shape[1] // 2
    return (jax.nn.silu(total[:, :half]) * total[:, half:]).astype(jnp.bfloat16)


def estimate(flops):
    return pl.CostEstimate(flops=flops, bytes_accessed=flops // 400, transcendentals=0)


def copies_call(body, y, arrays, shapes, stages):
    scratch = [pltpu.VMEM(s, jnp.bfloat16) for s in stages]
    return pl.pallas_call(
        body,
        in_specs=[pl.BlockSpec(memory_space=pltpu.SMEM)] + [pl.BlockSpec(memory_space=pl.ANY)] * len(arrays),
        out_specs=[pl.BlockSpec(memory_space=pl.ANY)] * len(shapes),
        out_shape=[jax.ShapeDtypeStruct(s, jnp.bfloat16) for s in shapes],
        scratch_shapes=[*scratch, pltpu.SemaphoreType.DMA((2, len(stages)))],
        cost_estimate=estimate(10**9),
        compiler_params=pltpu.CompilerParams(vmem_limit_bytes=60 * 1024 * 1024),
    )(y[None], *arrays)


def run_copies(pairs, stages, sems):
    first = [pltpu.make_async_copy(src, stage, sems.at[0, n]) for n, ((src, _), stage) in enumerate(zip(pairs, stages))]
    second = [pltpu.make_async_copy(stage, dst, sems.at[1, n]) for n, ((_, dst), stage) in enumerate(zip(pairs, stages))]
    for copy in first:
        copy.start()
    for one, two in zip(first, second):
        one.wait()
        two.start()
    for copy in second:
        copy.wait()


def blocks_of(y, w, out, at, count, width):
    pairs = []
    for x in range(count):
        rows = pl.ds(pl.multiple_of((2 * x + y) * width, width), width)
        pairs.append((w.at[rows, :], out.at[pl.ds(at + x * width, width), :]))
    return pairs


def columns_of(y, w, out, count, width):
    pairs = []
    for x in range(count):
        lanes = pl.ds(pl.multiple_of((2 * x + y) * width, width), width)
        pairs.append((w.at[:, lanes], out.at[:, pl.ds(x * width, width)]))
    return pairs


def rows_for_neighbour(y, w_gate, w_up, lines, count, width):
    def body(y_ref, g, u, t, first, second, *rest):
        other = 1 - y_ref[0]
        pairs = [(t, first.at[pl.ds(count * width, lines.shape[0]), :])]
        pairs += blocks_of(other, g, first, 0, count, width) + blocks_of(other, u, second, 0, count, width)
        run_copies(pairs, rest[:-1], rest[-1])

    hidden = w_gate.shape[1]
    shapes = [(count * width + lines.shape[0], hidden), (count * width, hidden)]
    stages = [lines.shape] + [(width, hidden)] * (2 * count)
    return copies_call(body, y, (w_gate, w_up, lines), shapes, stages)


def own_blocks(y, w_gate, w_up, w_down, count, width):
    def body(y_ref, g, u, d, out, near, far, *rest):
        y = y_ref[0]
        pairs = blocks_of(y, g, out, 0, count, width) + blocks_of(y, u, out, count * width, count, width)
        pairs += columns_of(y, d, near, count, width) + columns_of(1 - y, d, far, count, width)
        run_copies(pairs, rest[:-1], rest[-1])

    hidden = w_gate.shape[1]
    shapes = [(2 * count * width, hidden), (hidden, count * width), (hidden, count * width)]
    stages = [(width, hidden)] * (2 * count) + [(hidden, width)] * (2 * count)
    return copies_call(body, y, (w_gate, w_up, w_down), shapes, stages)


def partial_sums(x, gates, ups):
    chips, chunks, rows, _ = x.shape
    ins = (*gates, *ups)
    hidden = ins[0].shape[1]
    width = chunks * LANES
    wide = len(ins) * hidden

    def body(x_ref, *refs):
        w, acc, sent = refs[: len(ins)], refs[-2], refs[-1]
        i = pl.program_id(0)

        @pl.when(i == 0)
        def _():
            acc[...] = jnp.zeros_like(acc)

        lines = jnp.concatenate([x_ref[0, j] for j in range(chunks)], axis=1)
        weights = jnp.concatenate([r[...] for r in w], axis=1)
        acc[...] += jnp.dot(lines, weights, preferred_element_type=jnp.float32)

        @pl.when(i == chips - 1)
        def _():
            sent[...] = acc[...].astype(sent.dtype)

    whole = pl.BlockSpec((rows, wide), lambda i: (0, 0))
    return pl.pallas_call(
        body,
        grid=(chips,),
        in_specs=[pl.BlockSpec((1, chunks, rows, LANES), lambda i: (i, 0, 0, 0))]
        + [pl.BlockSpec((width, hidden), lambda i: (i, 0))] * len(gates)
        + [pl.BlockSpec((width, hidden), lambda i: (chips + i, 0))] * 2
        + [pl.BlockSpec((width, hidden), lambda i: (i, 0))] * 2,
        out_specs=[whole, whole],
        out_shape=[
            jax.ShapeDtypeStruct((rows, wide), jnp.float32),
            jax.ShapeDtypeStruct((rows, wide), jnp.bfloat16),
        ],
        cost_estimate=estimate(2 * rows * chips * width * wide),
        compiler_params=PARAMS,
        name="partial",
    )(x, *ins)


def down(sums, other, outs, count, chunks):
    rows, wide = sums.shape
    part = outs[0].shape[0]
    width = chunks * LANES

    def body(s_ref, o_ref, *refs):
        w, out, h = refs[: len(outs)], refs[-2], refs[-1]

        @pl.when(pl.program_id(0) == 0)
        def _():
            theirs = o_ref[...].astype(jnp.float32)
            quarter = wide // 4
            order = [1, 0, 3, 2]
            theirs = jnp.concatenate([theirs[:, q * quarter : (q + 1) * quarter] for q in order], axis=1)
            h[...] = activate(s_ref[...] + theirs)

        weights = jnp.concatenate([r[...] for r in w], axis=0)
        result = jnp.dot(h[...], weights, preferred_element_type=jnp.float32)
        for j in range(chunks):
            out[0, j] = result[:, j * LANES : (j + 1) * LANES].astype(out.dtype)

    whole = pl.BlockSpec((rows, wide), lambda i: (0, 0))
    return pl.pallas_call(
        body,
        grid=(count,),
        in_specs=[whole, whole] + [pl.BlockSpec((part, width), lambda i: (0, i))] * len(outs),
        out_specs=pl.BlockSpec((1, chunks, rows, LANES), lambda i: (i, 0, 0, 0)),
        out_shape=jax.ShapeDtypeStruct((count, chunks, rows, LANES), jnp.bfloat16),
        scratch_shapes=[pltpu.VMEM((rows, wide // 2), jnp.bfloat16)],
        cost_estimate=estimate(2 * rows * count * width * 4 * part),
        compiler_params=SMALL,
        name="down",
    )(sums, other, *outs)


def shared_expert(x, rest, at, w_gate, w_up, w_down):
    half, ys, chunks, rows, _ = x.shape
    pairs = 2 * half
    hidden = w_gate.shape[1]
    width = ys * chunks * LANES

    def body(_, x_ref, r_ref, g_ref, u_ref, d_ref, out, acc, h):
        i = pl.program_id(0)

        @pl.when(i == 0)
        def _():
            acc[...] = jnp.zeros_like(acc)

        def add(ref):
            lines = jnp.concatenate([ref[0, y, j] for y in range(ys) for j in range(chunks)], axis=1)
            weights = jnp.concatenate([g_ref[...], u_ref[...]], axis=1)
            acc[...] += jnp.dot(lines, weights, preferred_element_type=jnp.float32)

        @pl.when(i < half)
        def _():
            add(x_ref)

        @pl.when((i >= half) & (i < pairs))
        def _():
            add(r_ref)

        @pl.when(i == pairs)
        def _():
            h[...] = activate(acc[...])

        @pl.when(i >= pairs)
        def _():
            result = jnp.dot(h[...], d_ref[...], preferred_element_type=jnp.float32)
            for y in range(ys):
                for j in range(chunks):
                    lane = (y * chunks + j) * LANES
                    out[0, y, j] = result[:, lane : lane + LANES].astype(out.dtype)

    first = lambda i: jnp.minimum(i, pairs - 1)
    second = lambda i: jnp.maximum(i - pairs, 0)
    w_in = pl.BlockSpec((width, hidden), lambda i, at: (at[first(i)], 0))
    block = (1, ys, chunks, rows, LANES)
    return pl.pallas_call(
        body,
        grid_spec=pltpu.PrefetchScalarGridSpec(
            num_scalar_prefetch=1,
            grid=(2 * pairs,),
            in_specs=[
                pl.BlockSpec(block, lambda i, at: (jnp.minimum(i, half - 1), 0, 0, 0, 0)),
                pl.BlockSpec(block, lambda i, at: (jnp.clip(i - half, 0, half - 1), 0, 0, 0, 0)),
                w_in,
                w_in,
                pl.BlockSpec((hidden, width), lambda i, at: (0, at[second(i)])),
            ],
            out_specs=pl.BlockSpec(block, lambda i, at: (second(i), 0, 0, 0, 0)),
            scratch_shapes=[pltpu.VMEM((rows, 2 * hidden), jnp.float32), pltpu.VMEM((rows, hidden), jnp.bfloat16)],
        ),
        out_shape=jax.ShapeDtypeStruct((pairs, *x.shape[1:]), jnp.bfloat16),
        cost_estimate=estimate(6 * rows * pairs * width * hidden),
        compiler_params=PARAMS,
        name="shared",
    )(at, x, rest, w_gate, w_up, w_down)


def local(
    tokens,
    expert_ids,
    gate_scores,
    routed_gate,
    routed_up,
    routed_down,
    shared_gate,
    shared_up,
    shared_down,
):
    experts = routed_gate.shape[0] * lax.axis_size("ep")
    xs = lax.axis_size("x")
    core, xi, yi = lax.axis_index("c"), lax.axis_index("x"), lax.axis_index("y")
    row_count, top_count = expert_ids.shape
    capacity = min(row_count, row_count * top_count * 15 // (8 * experts))
    slots = capacity // 2
    swap = [(0, 1), (1, 0)]

    def to_y(v):
        return lax.ppermute(v, "y", swap)

    def to_x(v, bit):
        return lax.ppermute(v, "x", [(i, i ^ bit) for i in range(xs)])

    def to_c(v):
        return lax.ppermute(v, "c", swap)

    def halve(v, bit):
        half = v.shape[0] // 2
        return (v[:half].astype(jnp.float32) + to_x(v[half:], bit).astype(jnp.float32)).astype(v.dtype)

    def exchange(v, axes):
        return lax.all_to_all(v, axes, split_axis=0, concat_axis=0, tiled=True)

    chunks = 2 * tokens.shape[1] // LANES
    used = chunks * slots
    message = -(-used // 8) * 8
    columns = chunks * row_count
    routed_rows = slots * experts
    width = chunks * LANES

    pair = lax.all_gather(tokens, "c", axis=1, tiled=True)
    stacked = jnp.moveaxis(pair.reshape(row_count, chunks, LANES), 1, 0)
    slot, score = slot_table(expert_ids, gate_scores, experts, chunks)
    place = jnp.arange(message, dtype=jnp.int32)[:, None]
    column = jnp.arange(columns, dtype=jnp.int32)[None, :]
    fits = (place // slots == column // row_count) & (place < used)
    target = jnp.where(fits, place % slots + slots * core, -1024)
    match = slot[:, None, :] == target[None, :, :]
    select = match.astype(jnp.bfloat16).reshape(experts * message, columns)
    buckets = jnp.dot(select, stacked.reshape(columns, LANES), preferred_element_type=jnp.float32)
    buckets = buckets.astype(jnp.bfloat16).reshape(experts, message, LANES)
    w_gate, w_up, w_down = routed_gate[0], routed_up[0], routed_down[0]
    received = exchange(buckets, "ep")
    _, w_gate, w_up, w_down, lines = lax.optimization_barrier(
        (buckets, w_gate, w_up, w_down, stacked.reshape(columns, LANES))
    )
    other, other_up = rows_for_neighbour(yi, w_gate, w_up, lines, xs, width)
    got = to_y(other)
    got_up = to_y(other_up)
    mine, mine_down, other_down = own_blocks(yi, w_gate, w_up, w_down, xs, width)
    partner = to_c(mine)
    partner_down = to_c(mine_down)
    received, partner, partner_down = lax.optimization_barrier((received, partner, partner_down))
    rows = jnp.swapaxes(received, 0, 1)[:used].reshape(chunks, routed_rows, LANES)
    gathered = exchange(jnp.broadcast_to(rows[None], (xs,) + rows.shape), "x")
    got_down = to_y(other_down)
    partner_got = to_c(got)
    theirs = got[xs * width :].reshape(stacked.shape)
    whole = jnp.where(yi == 0, jnp.stack([stacked, theirs]), jnp.stack([theirs, stacked]))[None]
    whole_x = to_x(whole, 2)
    partner_got_up = to_c(got_up)
    gathered, partner_got, partner_got_up = lax.optimization_barrier((gathered, partner_got, partner_got_up))
    sums, sent = partial_sums(
        gathered, (mine, partner, got, partner_got), (mine, partner, got_up, partner_got_up)
    )
    other_sums = to_y(sent)
    whole = jnp.concatenate([whole, whole_x], axis=0)
    rest = to_x(whole, 1)
    partner_got_down = to_c(got_down)
    other_sums, partner_got_down, rest = lax.optimization_barrier((other_sums, partner_got_down, rest))
    products = down(sums, other_sums, (mine_down, partner_down, got_down, partner_got_down), xs, chunks)
    reduced = exchange(products, "x")
    at = jnp.bitwise_xor(jnp.array([0, 2, 1, 3], jnp.int32), xi)
    part = shared_expert(whole, rest, at, shared_gate, shared_up, shared_down)
    far = to_x(part[2:], 1)
    reduced, part = lax.optimization_barrier((reduced, part))
    total = jnp.sum(reduced.astype(jnp.float32), axis=0).astype(jnp.bfloat16)
    outcome = jnp.pad(total.reshape(used, experts, LANES), ((0, message - used), (0, 0), (0, 0)))
    returned = exchange(jnp.swapaxes(outcome, 0, 1), "ep")
    part = (part[:2].astype(jnp.float32) + far.astype(jnp.float32)).astype(part.dtype)
    part = halve(part, 2)[0]
    kept = jnp.where(yi == 0, part[0], part[1])
    lost = jnp.where(yi == 0, part[1], part[0])
    shared = kept.astype(jnp.float32) + to_y(lost).astype(jnp.float32)
    returned, shared = lax.optimization_barrier((returned, shared))

    returned = returned.reshape(experts * message, LANES)
    weights = jnp.where(match, score[:, None, :], 0.0).reshape(experts * message, columns)
    routed = lax.dot_general(
        weights,
        returned.astype(jnp.float32),
        (((0,), (0,)), ((), ())),
        precision=lax.Precision.HIGHEST,
        preferred_element_type=jnp.float32,
    )
    both = (routed.reshape(shared.shape) + shared).reshape(2, chunks // 2, row_count, LANES)
    keep = jnp.where(core == 0, both[0], both[1])
    send = jnp.where(core == 0, both[1], both[0])
    result = keep + lax.ppermute(send, "c", swap)
    return jnp.moveaxis(result, 0, 1).reshape(row_count, tokens.shape[1]).astype(jnp.bfloat16)


def solution(mesh):
    ep, tp = mesh.shape["ep"], mesh.shape["tp"]
    fine = Mesh(mesh.devices.reshape(ep, tp // 4, 2, 2), ("ep", "x", "y", "c"))
    tp_axes = ("x", "y", "c")
    placed = (
        P("ep", tp_axes),
        P("ep", None),
        P("ep", None),
        P("ep", None, tp_axes),
        P("ep", None, tp_axes),
        P("ep", tp_axes, None),
        P(None, tp_axes),
        P(None, tp_axes),
        P(tp_axes, None),
    )
    return jax.shard_map(
        local, mesh=fine, in_specs=placed, out_specs=P("ep", tp_axes), check_vma=False
    )
```

```python
import jax
import jax.numpy as jnp
from jax import lax
from jax.experimental import pallas as pl
from jax.experimental.pallas import tpu as pltpu
from jax.sharding import Mesh
from jax.sharding import PartitionSpec as P


LANES = 128
SMALL = pltpu.CompilerParams(dimension_semantics=("arbitrary",), vmem_limit_bytes=24 * 1024 * 1024)
PARAMS = pltpu.CompilerParams(dimension_semantics=("arbitrary",), vmem_limit_bytes=60 * 1024 * 1024)


def slot_table(expert_ids, gate_scores, experts, copies):
    rows = expert_ids.shape[0]
    hit = expert_ids.T[None, :, :] == jnp.arange(experts, dtype=jnp.int32)[:, None, None]
    named = jnp.sum(hit.astype(jnp.float32), axis=1)
    score = jnp.sum(jnp.where(hit, gate_scores.T[None, :, :], 0.0), axis=1)
    earlier = jnp.arange(rows)[:, None] < jnp.arange(rows)[None, :]
    same = jnp.arange(rows)[:, None] == jnp.arange(rows)[None, :]
    weight = jnp.tile(earlier.astype(jnp.bfloat16) + 128 * same.astype(jnp.bfloat16), (1, copies))
    slot = jnp.dot(named.astype(jnp.bfloat16), weight, preferred_element_type=jnp.float32) - 128
    return slot.astype(jnp.int32), jnp.tile(score, (1, copies))


def activate(total):
    half = total.shape[1] // 2
    return (jax.nn.silu(total[:, :half]) * total[:, half:]).astype(jnp.bfloat16)


def estimate(flops):
    return pl.CostEstimate(flops=flops, bytes_accessed=flops // 400, transcendentals=0)


def copies_call(body, y, arrays, shapes, stages):
    scratch = [pltpu.VMEM(s, jnp.bfloat16) for s in stages]
    return pl.pallas_call(
        body,
        in_specs=[pl.BlockSpec(memory_space=pltpu.SMEM)] + [pl.BlockSpec(memory_space=pl.ANY)] * len(arrays),
        out_specs=[pl.BlockSpec(memory_space=pl.ANY)] * len(shapes),
        out_shape=[jax.ShapeDtypeStruct(s, jnp.bfloat16) for s in shapes],
        scratch_shapes=[*scratch, pltpu.SemaphoreType.DMA((2, len(stages)))],
        cost_estimate=estimate(10**9),
        compiler_params=pltpu.CompilerParams(vmem_limit_bytes=60 * 1024 * 1024),
    )(y[None], *arrays)


def run_copies(pairs, stages, sems):
    first = [pltpu.make_async_copy(src, stage, sems.at[0, n]) for n, ((src, _), stage) in enumerate(zip(pairs, stages))]
    second = [pltpu.make_async_copy(stage, dst, sems.at[1, n]) for n, ((_, dst), stage) in enumerate(zip(pairs, stages))]
    for copy in first:
        copy.start()
    for one, two in zip(first, second):
        one.wait()
        two.start()
    for copy in second:
        copy.wait()


def blocks_of(y, w, out, at, count, width):
    pairs = []
    for x in range(count):
        rows = pl.ds(pl.multiple_of((2 * x + y) * width, width), width)
        pairs.append((w.at[rows, :], out.at[pl.ds(at + x * width, width), :]))
    return pairs


def columns_of(y, w, out, count, width):
    pairs = []
    for x in range(count):
        lanes = pl.ds(pl.multiple_of((2 * x + y) * width, width), width)
        pairs.append((w.at[:, lanes], out.at[:, pl.ds(x * width, width)]))
    return pairs


def rows_for_neighbour(y, w_gate, w_up, lines, count, width):
    def body(y_ref, g, u, t, first, second, *rest):
        other = 1 - y_ref[0]
        pairs = [(t, first.at[pl.ds(count * width, lines.shape[0]), :])]
        pairs += blocks_of(other, g, first, 0, count, width) + blocks_of(other, u, second, 0, count, width)
        run_copies(pairs, rest[:-1], rest[-1])

    hidden = w_gate.shape[1]
    shapes = [(count * width + lines.shape[0], hidden), (count * width, hidden)]
    stages = [lines.shape] + [(width, hidden)] * (2 * count)
    return copies_call(body, y, (w_gate, w_up, lines), shapes, stages)


def own_blocks(y, w_gate, w_up, w_down, count, width):
    def body(y_ref, g, u, d, out, near, far, *rest):
        y = y_ref[0]
        pairs = blocks_of(y, g, out, 0, count, width) + blocks_of(y, u, out, count * width, count, width)
        pairs += columns_of(y, d, near, count, width) + columns_of(1 - y, d, far, count, width)
        run_copies(pairs, rest[:-1], rest[-1])

    hidden = w_gate.shape[1]
    shapes = [(2 * count * width, hidden), (hidden, count * width), (hidden, count * width)]
    stages = [(width, hidden)] * (2 * count) + [(hidden, width)] * (2 * count)
    return copies_call(body, y, (w_gate, w_up, w_down), shapes, stages)


def partial_sums(x, gates, ups):
    chips, chunks, rows, _ = x.shape
    ins = (*gates, *ups)
    hidden = ins[0].shape[1]
    width = chunks * LANES
    wide = len(ins) * hidden

    def body(x_ref, *refs):
        w, acc, sent = refs[: len(ins)], refs[-2], refs[-1]
        i = pl.program_id(0)

        lines = jnp.concatenate([x_ref[0, j] for j in range(chunks)], axis=1)
        weights = jnp.concatenate([r[...] for r in w], axis=1)
        step = jnp.dot(lines, weights, preferred_element_type=jnp.float32)

        @pl.when(i == 0)
        def _():
            acc[...] = step

        @pl.when(i > 0)
        def _():
            acc[...] += step

        @pl.when(i == chips - 1)
        def _():
            sent[...] = acc[...].astype(sent.dtype)

    whole = pl.BlockSpec((rows, wide), lambda i: (0, 0))
    return pl.pallas_call(
        body,
        grid=(chips,),
        in_specs=[pl.BlockSpec((1, chunks, rows, LANES), lambda i: (i, 0, 0, 0))]
        + [pl.BlockSpec((width, hidden), lambda i: (i, 0))] * len(gates)
        + [pl.BlockSpec((width, hidden), lambda i: (chips + i, 0))] * 2
        + [pl.BlockSpec((width, hidden), lambda i: (i, 0))] * 2,
        out_specs=[whole, whole],
        out_shape=[
            jax.ShapeDtypeStruct((rows, wide), jnp.float32),
            jax.ShapeDtypeStruct((rows, wide), jnp.bfloat16),
        ],
        cost_estimate=estimate(2 * rows * chips * width * wide),
        compiler_params=SMALL,
        name="partial",
    )(x, *ins)


def down(sums, other, outs, count, chunks):
    rows, wide = sums.shape
    part = outs[0].shape[0]
    width = chunks * LANES

    def body(s_ref, o_ref, *refs):
        w, out, h = refs[: len(outs)], refs[-2], refs[-1]

        @pl.when(pl.program_id(0) == 0)
        def _():
            theirs = o_ref[...].astype(jnp.float32)
            quarter = wide // 4
            order = [1, 0, 3, 2]
            theirs = jnp.concatenate([theirs[:, q * quarter : (q + 1) * quarter] for q in order], axis=1)
            h[...] = activate(s_ref[...] + theirs)

        weights = jnp.concatenate([r[...] for r in w], axis=0)
        result = jnp.dot(h[...], weights, preferred_element_type=jnp.float32)
        for j in range(chunks):
            out[0, j] = result[:, j * LANES : (j + 1) * LANES].astype(out.dtype)

    whole = pl.BlockSpec((rows, wide), lambda i: (0, 0))
    return pl.pallas_call(
        body,
        grid=(count,),
        in_specs=[whole, whole] + [pl.BlockSpec((part, width), lambda i: (0, i))] * len(outs),
        out_specs=pl.BlockSpec((1, chunks, rows, LANES), lambda i: (i, 0, 0, 0)),
        out_shape=jax.ShapeDtypeStruct((count, chunks, rows, LANES), jnp.bfloat16),
        scratch_shapes=[pltpu.VMEM((rows, wide // 2), jnp.bfloat16)],
        cost_estimate=estimate(2 * rows * count * width * 4 * part),
        compiler_params=SMALL,
        name="down",
    )(sums, other, *outs)


def shared_expert(x, rest, at, w_gate, w_up, w_down):
    half, ys, chunks, rows, _ = x.shape
    pairs = 2 * half
    hidden = w_gate.shape[1]
    width = ys * chunks * LANES

    def body(_, x_ref, r_ref, g_ref, u_ref, d_ref, out, acc, h):
        i = pl.program_id(0)

        @pl.when(i == 0)
        def _():
            acc[...] = jnp.zeros_like(acc)

        def add(ref):
            lines = jnp.concatenate([ref[0, y, j] for y in range(ys) for j in range(chunks)], axis=1)
            weights = jnp.concatenate([g_ref[...], u_ref[...]], axis=1)
            acc[...] += jnp.dot(lines, weights, preferred_element_type=jnp.float32)

        @pl.when(i < half)
        def _():
            add(x_ref)

        @pl.when((i >= half) & (i < pairs))
        def _():
            add(r_ref)

        @pl.when(i == pairs)
        def _():
            h[...] = activate(acc[...])

        @pl.when(i >= pairs)
        def _():
            result = jnp.dot(h[...], d_ref[...], preferred_element_type=jnp.float32)
            for y in range(ys):
                for j in range(chunks):
                    lane = (y * chunks + j) * LANES
                    out[0, y, j] = result[:, lane : lane + LANES].astype(out.dtype)

    first = lambda i: jnp.minimum(i, pairs - 1)
    second = lambda i: jnp.maximum(i - pairs, 0)
    w_in = pl.BlockSpec((width, hidden), lambda i, at: (at[first(i)], 0))
    block = (1, ys, chunks, rows, LANES)
    return pl.pallas_call(
        body,
        grid_spec=pltpu.PrefetchScalarGridSpec(
            num_scalar_prefetch=1,
            grid=(2 * pairs,),
            in_specs=[
                pl.BlockSpec(block, lambda i, at: (jnp.minimum(i, half - 1), 0, 0, 0, 0)),
                pl.BlockSpec(block, lambda i, at: (jnp.clip(i - half, 0, half - 1), 0, 0, 0, 0)),
                w_in,
                w_in,
                pl.BlockSpec((hidden, width), lambda i, at: (0, at[second(i)])),
            ],
            out_specs=pl.BlockSpec(block, lambda i, at: (second(i), 0, 0, 0, 0)),
            scratch_shapes=[pltpu.VMEM((rows, 2 * hidden), jnp.float32), pltpu.VMEM((rows, hidden), jnp.bfloat16)],
        ),
        out_shape=jax.ShapeDtypeStruct((pairs, *x.shape[1:]), jnp.bfloat16),
        cost_estimate=estimate(6 * rows * pairs * width * hidden),
        compiler_params=PARAMS,
        name="shared",
    )(at, x, rest, w_gate, w_up, w_down)


def local(
    tokens,
    expert_ids,
    gate_scores,
    routed_gate,
    routed_up,
    routed_down,
    shared_gate,
    shared_up,
    shared_down,
):
    experts = routed_gate.shape[0] * lax.axis_size("ep")
    xs = lax.axis_size("x")
    core, xi, yi = lax.axis_index("c"), lax.axis_index("x"), lax.axis_index("y")
    row_count, top_count = expert_ids.shape
    capacity = min(row_count, row_count * top_count * 15 // (8 * experts))
    slots = capacity // 2
    swap = [(0, 1), (1, 0)]

    def to_y(v):
        return lax.ppermute(v, "y", swap)

    def to_x(v, bit):
        return lax.ppermute(v, "x", [(i, i ^ bit) for i in range(xs)])

    def to_c(v):
        return lax.ppermute(v, "c", swap)

    def halve(v, bit):
        half = v.shape[0] // 2
        return (v[:half].astype(jnp.float32) + to_x(v[half:], bit).astype(jnp.float32)).astype(v.dtype)

    def exchange(v, axes):
        return lax.all_to_all(v, axes, split_axis=0, concat_axis=0, tiled=True)

    chunks = 2 * tokens.shape[1] // LANES
    used = chunks * slots
    message = -(-used // 8) * 8
    columns = chunks * row_count
    routed_rows = slots * experts
    width = chunks * LANES

    pair = lax.all_gather(tokens, "c", axis=1, tiled=True)
    stacked = jnp.moveaxis(pair.reshape(row_count, chunks, LANES), 1, 0)
    slot, score = slot_table(expert_ids, gate_scores, experts, chunks)
    place = jnp.arange(message, dtype=jnp.int32)[:, None]
    column = jnp.arange(columns, dtype=jnp.int32)[None, :]
    fits = (place // slots == column // row_count) & (place < used)
    target = jnp.where(fits, place % slots + slots * core, -1024)
    match = slot[:, None, :] == target[None, :, :]
    select = match.astype(jnp.bfloat16).reshape(experts * message, columns)
    buckets = jnp.dot(select, stacked.reshape(columns, LANES), preferred_element_type=jnp.float32)
    buckets = buckets.astype(jnp.bfloat16).reshape(experts, message, LANES)
    w_gate, w_up, w_down = routed_gate[0], routed_up[0], routed_down[0]
    received = exchange(buckets, "ep")
    _, w_gate, w_up, w_down, lines = lax.optimization_barrier(
        (buckets, w_gate, w_up, w_down, stacked.reshape(columns, LANES))
    )
    other, other_up = rows_for_neighbour(yi, w_gate, w_up, lines, xs, width)
    got = to_y(other)
    got_up = to_y(other_up)
    mine, mine_down, other_down = own_blocks(yi, w_gate, w_up, w_down, xs, width)
    partner = to_c(mine)
    partner_down = to_c(mine_down)
    received, partner, partner_down = lax.optimization_barrier((received, partner, partner_down))
    rows = jnp.swapaxes(received, 0, 1)[:used].reshape(chunks, routed_rows, LANES)
    gathered = exchange(jnp.broadcast_to(rows[None], (xs,) + rows.shape), "x")
    got_down = to_y(other_down)
    partner_got = to_c(got)
    theirs = got[xs * width :].reshape(stacked.shape)
    whole = jnp.where(yi == 0, jnp.stack([stacked, theirs]), jnp.stack([theirs, stacked]))[None]
    whole_x = to_x(whole, 2)
    got_up, partner_got = lax.optimization_barrier((got_up, partner_got))
    partner_got_up = to_c(got_up)
    gathered, partner_got, partner_got_up = lax.optimization_barrier((gathered, partner_got, partner_got_up))
    sums, sent = partial_sums(
        gathered, (mine, partner, got, partner_got), (mine, partner, got_up, partner_got_up)
    )
    other_sums = to_y(sent)
    whole = jnp.concatenate([whole, whole_x], axis=0)
    rest = to_x(whole, 1)
    partner_got_down = to_c(got_down)
    other_sums, partner_got_down, rest = lax.optimization_barrier((other_sums, partner_got_down, rest))
    products = down(sums, other_sums, (mine_down, partner_down, got_down, partner_got_down), xs, chunks)
    reduced = exchange(products, "x")
    at = jnp.bitwise_xor(jnp.array([0, 2, 1, 3], jnp.int32), xi)
    part = shared_expert(whole, rest, at, shared_gate, shared_up, shared_down)
    far = to_x(part[2:], 1)
    reduced, part = lax.optimization_barrier((reduced, part))
    total = jnp.sum(reduced.astype(jnp.float32), axis=0).astype(jnp.bfloat16)
    outcome = jnp.pad(total.reshape(used, experts, LANES), ((0, message - used), (0, 0), (0, 0)))
    returned = exchange(jnp.swapaxes(outcome, 0, 1), "ep")
    part = (part[:2].astype(jnp.float32) + far.astype(jnp.float32)).astype(part.dtype)
    part = halve(part, 2)[0]
    kept = jnp.where(yi == 0, part[0], part[1])
    lost = jnp.where(yi == 0, part[1], part[0])
    shared = kept.astype(jnp.float32) + to_y(lost).astype(jnp.float32)
    returned, shared = lax.optimization_barrier((returned, shared))

    returned = returned.reshape(experts * message, LANES)
    weights = jnp.where(match, score[:, None, :], 0.0).reshape(experts * message, columns)
    routed = lax.dot_general(
        weights,
        returned.astype(jnp.float32),
        (((0,), (0,)), ((), ())),
        precision=lax.Precision.HIGHEST,
        preferred_element_type=jnp.float32,
    )
    both = (routed.reshape(shared.shape) + shared).reshape(2, chunks // 2, row_count, LANES)
    keep = jnp.where(core == 0, both[0], both[1])
    send = jnp.where(core == 0, both[1], both[0])
    result = keep + lax.ppermute(send, "c", swap)
    return jnp.moveaxis(result, 0, 1).reshape(row_count, tokens.shape[1]).astype(jnp.bfloat16)


def solution(mesh):
    ep, tp = mesh.shape["ep"], mesh.shape["tp"]
    fine = Mesh(mesh.devices.reshape(ep, tp // 4, 2, 2), ("ep", "x", "y", "c"))
    tp_axes = ("x", "y", "c")
    placed = (
        P("ep", tp_axes),
        P("ep", None),
        P("ep", None),
        P("ep", None, tp_axes),
        P("ep", None, tp_axes),
        P("ep", tp_axes, None),
        P(None, tp_axes),
        P(None, tp_axes),
        P(tp_axes, None),
    )
    return jax.shard_map(
        local, mesh=fine, in_specs=placed, out_specs=P("ep", tp_axes), check_vma=False
    )
```
